32 devices in a mesh: batch: 4 (over y, core), tm: 2 (over x), space: 4 (over z).
Axes of the slice: x: 2, y: 2, z: 4, core: 2. Of those that a mesh axis runs over, the one named last changes fastest.
Arguments:
- clip_tokens: bfloat16 [4, 4, 32, 32, 1024], P('batch', None, 'space', 'tm'), may hold values from -6 to 6
- frame_order: int32 [4, 4], P('batch'), may hold values from 0 to 3, each once within a row
- row_reach: int32 [4, 4], P('batch', 'tm'), may hold values from 1 to 4
- spatial_gain: float32 [1024], replicated, may hold values from 0.1 to 1.9
- spatial_heads: bfloat16 [1024, 3072], replicated, may hold values from -2 to 2
- spatial_merge: bfloat16 [1024, 1024], replicated, may hold values from -0.1875 to 0.1875
- temporal_gain: float32 [1024], replicated, may hold values from 0.1 to 1.9
- temporal_heads: bfloat16 [1024, 3072], replicated, may hold values from -2 to 2
- temporal_merge: bfloat16 [1024, 1024], replicated, may hold values from -0.1875 to 0.1875
- cotangent: bfloat16 [4, 4, 32, 32, 1024], P('batch', 'tm', 'space'), may hold values from -0.059814453 to 0.059814453
Outputs:
- output: bfloat16 [4, 4, 32, 32, 1024], P('batch', 'tm', 'space')
- weight_grad: float32 [1024, 1024], P(('tm', 'space'))
The draws below stay inside these ranges and needn't reach their ends.
Inputs may be any that keep to these rules, and one draw needn't show every extreme that they name: Each row of frame_order names every number from 0 to 3 once.
All inputs are finite; a program needn't handle non-finite values.
Results may differ from the reference program's by a relative error of at most 0.025.
Values may be sent and summed in bfloat16 or wider, within the bound.
A program may use at most 128 MiB of HBM per device.

```python
import jax
import jax.numpy as jnp
from jax import lax

COLS = 32
HALO = 4
D = 1024
HEADS = 16
HEAD_DIM = 64
CLIPS = 4
FRAMES = 4
ROWS = 32


def projection_draw(key):
    key_one, key_two, key_three = jax.random.split(key, 3)
    plain_part = jnp.clip(jax.random.normal(key_one, (D, 3 * D), jnp.float32), -6.0, 6.0) * D ** (-0.5)
    return plain_part.astype(jnp.bfloat16)


def draw_spatial_heads(key, part):
    return projection_draw(jax.random.fold_in(key, 11))


def draw_temporal_heads(key, part):
    return projection_draw(jax.random.fold_in(key, 23))


def with_ends(drawn, own_key, smallest, high):
    index_at = [jax.random.randint(jax.random.fold_in(own_key, axis), (), 0, length) for axis, length in enumerate(drawn.shape)]
    longest = drawn.shape.index(max(drawn.shape))
    beside = index_at[:longest] + [(index_at[longest] + 1) % drawn.shape[longest]] + index_at[longest + 1:]
    return drawn.at[tuple(index_at)].set(smallest).at[tuple(beside)].set(high)


def block_levels(own_key, dims, cuts, low, high):
    factor_of, own = 1.0, jax.random.fold_in(own_key, 6)
    for dim, shards_of in cuts:
        steps = jnp.exp(jax.random.uniform(jax.random.fold_in(own, dim), (shards_of,), jnp.float32, low / len(cuts), high / len(cuts)))
        factor_of = factor_of * jnp.repeat(steps, dims[dim] // shards_of).reshape([-1 if axis == dim else 1 for axis in range(len(dims))])
    return factor_of


def gaussian(stream_key, extent, spread, bound, cuts=(), kind=jnp.bfloat16):
    entries = spread * jax.random.normal(stream_key, extent, jnp.float32)
    if cuts:
        entries = entries * block_levels(stream_key, extent, cuts, -0.22, 0.18)
    return jnp.clip(entries, -bound, bound).astype(kind)


def setup_inputs(seed: int = 0) -> dict:
    seeds = jax.random.split(jax.random.key(seed), 11)
    return {
        "clip_tokens": gaussian(seeds[0], (CLIPS, FRAMES, ROWS, COLS, D), 1.0, 6.0, ((0, 4), (2, 4), (3, 2))),
        "frame_order": jax.vmap(lambda own: jax.random.permutation(own, FRAMES))(jax.random.split(seeds[1], CLIPS)).reshape((CLIPS, FRAMES)).astype(jnp.int32),
        "row_reach": with_ends(jax.random.randint(seeds[2], (CLIPS, FRAMES), 1, HALO + 1), jax.random.fold_in(seeds[2], 1), 1, HALO).astype(jnp.int32),
        "spatial_gain": jnp.clip(1.0 + 0.18 * jax.random.normal(seeds[3], (D,), jnp.float32), 0.1, 1.9),
        "spatial_heads": draw_spatial_heads(jax.random.fold_in(seeds[10], 71), 0),
        "spatial_merge": gaussian(seeds[5], (D, D), D ** -0.5, 0.1875),
        "temporal_gain": jnp.clip(1.0 + 0.18 * jax.random.normal(seeds[6], (D,), jnp.float32), 0.1, 1.9),
        "temporal_heads": draw_temporal_heads(jax.random.fold_in(seeds[10], 71), 0),
        "temporal_merge": gaussian(seeds[8], (D, D), D ** -0.5, 0.1875),
        "cotangent": gaussian(seeds[9], (CLIPS, FRAMES, ROWS, COLS, D), 0.01, 0.059814453, ((0, 4), (1, 2), (2, 4))),
    }


floor_term = 0.5

def normalize(values, gain_vector):
    widened = values.astype(jnp.float32)
    scaled = widened * lax.rsqrt(lax.optimization_barrier(jnp.mean(widened * widened, axis=-1, keepdims=True)) + floor_term)
    return (scaled * gain_vector).astype(jnp.bfloat16)

def softmax_rounded(scores, allowed):
    masked = jnp.where(allowed, scores, -1e+30)
    top_score = lax.optimization_barrier(jnp.max(masked, axis=-1, keepdims=True))
    exponent = jnp.exp(masked - top_score)
    return (exponent / lax.optimization_barrier(jnp.sum(exponent, axis=-1, keepdims=True))).astype(jnp.bfloat16)

def spatial_frame(inputs):
    queries, keys_all, values_all, reach_now = inputs
    token_rows = jnp.arange(ROWS * COLS, dtype=jnp.int32) // COLS
    allowed = jnp.abs(token_rows[:, None] - token_rows[None, :]) <= reach_now
    query_heads = queries.astype(jnp.float32).reshape(-1, HEADS, HEAD_DIM)
    key_heads = keys_all.astype(jnp.float32).reshape(-1, HEADS, HEAD_DIM)
    value_heads = values_all.astype(jnp.float32).reshape(-1, HEADS, HEAD_DIM)
    scores = jnp.einsum('qhd,khd->hqk', query_heads, key_heads) * HEAD_DIM ** (-0.5)
    weights = softmax_rounded(scores, allowed[None])
    context = jnp.einsum('hqk,khd->qhd', weights.astype(jnp.float32), value_heads)
    return context.reshape(-1, D).astype(jnp.bfloat16)

def temporal_clip(queries, keys_all, values_all, order_row):
    query_heads = queries.astype(jnp.float32).reshape(FRAMES, -1, HEADS, HEAD_DIM)
    key_heads = keys_all.astype(jnp.float32).reshape(FRAMES, -1, HEADS, HEAD_DIM)
    value_heads = values_all.astype(jnp.float32).reshape(FRAMES, -1, HEADS, HEAD_DIM)
    scores = jnp.einsum('fthd,gthd->thfg', query_heads, key_heads) * HEAD_DIM ** (-0.5)
    allowed = order_row[None, :] <= order_row[:, None]
    weights = softmax_rounded(scores, allowed[None, None])
    context = jnp.einsum('thfg,gthd->fthd', weights.astype(jnp.float32), value_heads)
    return context.reshape(FRAMES, -1, D).astype(jnp.bfloat16)

def reference(clip_tokens, frame_order, row_reach, spatial_gain, spatial_heads, spatial_merge, temporal_gain, temporal_heads, temporal_merge, cotangent):
    tokens = ROWS * COLS

    def one_clip(running, inputs):
        frames_in, order_row, reach_row, cotangent_clip = inputs
        flat_input = frames_in.reshape(FRAMES, tokens, D)
        normed = normalize(flat_input, spatial_gain)
        projected = jnp.dot(normed, spatial_heads, preferred_element_type=jnp.float32).astype(jnp.bfloat16)
        spatial_context = lax.map(spatial_frame, (projected[..., :D], projected[..., D:2 * D], projected[..., 2 * D:], reach_row))
        middle = (flat_input.astype(jnp.float32) + jnp.dot(spatial_context, spatial_merge, preferred_element_type=jnp.float32)).astype(jnp.bfloat16)
        normed_two = normalize(middle, temporal_gain)
        projected_two = jnp.dot(normed_two, temporal_heads, preferred_element_type=jnp.float32).astype(jnp.bfloat16)
        temporal_context = temporal_clip(projected_two[..., :D], projected_two[..., D:2 * D], projected_two[..., 2 * D:], order_row)
        output_clip = (middle.astype(jnp.float32) + jnp.dot(temporal_context, temporal_merge, preferred_element_type=jnp.float32)).astype(jnp.bfloat16)
        gradient = running + lax.dot_general(temporal_context.reshape(-1, D), cotangent_clip.reshape(-1, D), (((0,), (0,)), ((), ())), preferred_element_type=jnp.float32)
        return (gradient, output_clip.reshape(FRAMES, ROWS, COLS, D))
    zero_grad = jnp.zeros((D, D), jnp.float32)
    weight_grad, output = lax.scan(one_clip, zero_grad, (clip_tokens, frame_order, row_reach, cotangent))
    return (output, weight_grad)
```

```python
import functools

import jax
import jax.numpy as jnp
from jax import lax
from jax.experimental import pallas as pl
from jax.experimental.pallas import tpu as pltpu
from jax.sharding import PartitionSpec as P

HALO = 4
HEADS = 16
HEAD_DIM = 64
LANES = 128
SCALE = HEAD_DIM ** (-0.5)
FLOOR = 0.5
BF = jnp.bfloat16
F32 = jnp.float32


def normalize(values, gain_vector):
    widened = values.astype(F32)
    scaled = widened * lax.rsqrt(jnp.mean(widened * widened, axis=-1, keepdims=True) + FLOOR)
    return (scaled * gain_vector).astype(BF)


def spatial_kernel(rows, cols, all_rows, reach_ref, first_ref, q_ref, k_ref, v_ref, kt_ref, vt_ref,
                   kb_ref, vb_ref, o_ref, kx, vx, bias):
    frame, block = pl.program_id(0), pl.program_id(1)
    span = HALO * cols
    window = 3 * span
    chunks = rows // HALO

    @pl.when(block == 0)
    def _():
        reach, first = reach_ref[frame], first_ref[0]
        for chunk in range(chunks):
            shape = (span, window)
            q_row = chunk * HALO + lax.broadcasted_iota(jnp.int32, shape, 0) // cols
            k_row = (chunk - 1) * HALO + lax.broadcasted_iota(jnp.int32, shape, 1) // cols
            place = first + k_row
            kept = (jnp.abs(k_row - q_row) <= reach) & (place >= 0) & (place < all_rows)
            bias[chunk] = jnp.where(kept, 0.0, -1e30)

    tokens = rows * cols
    for own, top, low, joined in ((k_ref, kt_ref, kb_ref, kx), (v_ref, vt_ref, vb_ref, vx)):
        joined[:span] = top[...]
        joined[span:span + tokens] = own[...]
        joined[span + tokens:] = low[...]

    lane = lax.broadcasted_iota(jnp.int32, (1, LANES), 1)
    first_head = (lane < HEAD_DIM).astype(F32)
    masks = (first_head.astype(BF), (1.0 - first_head).astype(BF))
    for pair in range(q_ref.shape[1] // LANES):
        at = slice(pair * LANES, (pair + 1) * LANES)
        for chunk in range(chunks):
            here = slice(chunk * span, (chunk + 1) * span)
            near = slice(chunk * span, chunk * span + window)
            q = q_ref[here, at] * BF(SCALE)
            k = kx[near, at]
            v = vx[near, at]
            outs = []
            for head in range(2):
                s = lax.dot_general(q * masks[head], k, (((1,), (1,)), ((), ())),
                                    preferred_element_type=F32) + bias[chunk]
                top_score = jnp.max(s, axis=-1, keepdims=True)
                p = jnp.exp(s - top_score).astype(BF)
                o = jnp.dot(p, v * masks[head] + masks[1 - head], preferred_element_type=F32)
                outs.append(o / pltpu.roll(o, HEAD_DIM, 1))
            o_ref[here, at] = jnp.where(lane < HEAD_DIM, outs[0], outs[1]).astype(BF)


def spatial_attend(projected, halo, reach, first_row, frames, rows, cols, all_rows):
    depth = projected.shape[1] // 3
    tokens, span = rows * cols, HALO * cols
    width = 2 * LANES
    blocks = depth // width
    here = lambda part: pl.BlockSpec((tokens, width), lambda f, j: (f, part * blocks + j))
    beside = lambda side, part: pl.BlockSpec(
        (span, width), lambda f, j: (side * frames + f, part * blocks + j))
    smem = pl.BlockSpec(memory_space=pltpu.SMEM)
    pairs = frames * HEADS * tokens * 3 * span
    return pl.pallas_call(
        functools.partial(spatial_kernel, rows, cols, all_rows),
        grid=(frames, blocks),
        out_shape=jax.ShapeDtypeStruct((frames * tokens, depth), BF),
        in_specs=[smem, smem, here(0), here(1), here(2), beside(0, 0), beside(0, 1), beside(1, 0), beside(1, 1)],
        out_specs=pl.BlockSpec((tokens, width), lambda f, j: (f, j)),
        scratch_shapes=[
            pltpu.VMEM((tokens + 2 * span, width), BF),
            pltpu.VMEM((tokens + 2 * span, width), BF),
            pltpu.VMEM((rows // HALO, span, 3 * span), F32),
        ],
        cost_estimate=pl.CostEstimate(flops=4 * pairs * LANES, bytes_accessed=frames * tokens * depth * 12,
                                      transcendentals=pairs),
        name="spatial",
    )(reach, first_row, projected, projected, projected, halo, halo, halo, halo)


def temporal_kernel(others, q_order, k_order, gather_ref, spread_ref, q_ref, *refs):
    k_refs, v_refs, o_ref = refs[:others + 1], refs[others + 1:2 * others + 2], refs[-1]
    frames = q_ref.shape[0]
    keys = [(ref, i) for ref in k_refs for i in range(frames)]
    values = [(ref, i) for ref in v_refs for i in range(frames)]
    for f in range(frames):
        q = q_ref[f] * BF(SCALE)
        scores = []
        for g, (ref, i) in enumerate(keys):
            s = jnp.dot(q * ref[i], gather_ref[...], preferred_element_type=F32)
            scores.append(s + jnp.where(k_order[g] <= q_order[f], 0.0, -1e30))
        top_score = functools.reduce(jnp.maximum, scores)
        exps = [jnp.exp(s - top_score) for s in scores]
        scale = 1.0 / functools.reduce(jnp.add, exps)
        total = None
        for g, (ref, i) in enumerate(values):
            w = jnp.dot((exps[g] * scale).astype(BF), spread_ref[...], preferred_element_type=F32)
            term = w * ref[i].astype(F32)
            total = term if total is None else total + term
        o_ref[f] = total.astype(BF)


def temporal_attend(own, others, q_order, k_order, frames):
    depth = own.shape[1] // 3
    tokens = own.shape[0] // frames
    size = min(tokens, 64)
    head = jnp.arange(depth, dtype=jnp.int32) // HEAD_DIM
    gather = (head[:, None] == jnp.arange(LANES, dtype=jnp.int32)[None, :]).astype(BF)
    own = own.reshape(frames, tokens, 3 * depth)
    others = [value.reshape(frames, tokens, 2 * depth) for value in others]
    part = lambda column: pl.BlockSpec((frames, size, depth), lambda i: (0, i, column))
    smem = pl.BlockSpec(memory_space=pltpu.SMEM)
    whole = lambda shape: pl.BlockSpec(shape, lambda i: (0, 0))
    count = len(others)
    keys = (count + 1) * frames
    out = pl.pallas_call(
        functools.partial(temporal_kernel, count),
        grid=(tokens // size,),
        out_shape=jax.ShapeDtypeStruct((frames, tokens, depth), BF),
        in_specs=[smem, smem, whole((depth, LANES)), whole((LANES, depth)), part(0)]
        + [part(1)] + [part(0)] * count + [part(2)] + [part(1)] * count,
        out_specs=part(0),
        cost_estimate=pl.CostEstimate(flops=4 * frames * keys * tokens * depth * LANES,
                                      bytes_accessed=4 * keys * tokens * depth, transcendentals=0),
        name="temporal",
    )(q_order, k_order, gather, gather.T, own, own, *others, own, *others)
    return out.reshape(frames * tokens, depth)


def cyclic(axis, shift):
    n = lax.axis_size(axis)
    return [(i, (i + shift) % n) for i in range(n)]


def exchange_bit(value, axis, bit):
    n = lax.axis_size(axis)
    return lax.ppermute(value, axis, [(i, i ^ bit) for i in range(n)])


def halve_columns(value, bit):
    half = value.shape[1] // 2
    mine = lax.axis_index("batch") // bit % 2
    sent = lax.dynamic_slice_in_dim(value, (1 - mine) * half, half, 1)
    kept = lax.dynamic_slice_in_dim(value, mine * half, half, 1)
    arrived = exchange_bit(sent, "batch", bit)
    return (kept.astype(F32) + arrived.astype(F32)).astype(BF)


def scatter_rows(value, axis):
    n, me = lax.axis_size(axis), lax.axis_index(axis)
    size = value.shape[0] // n
    take = lambda owner: lax.dynamic_slice_in_dim(value, owner * size, size, 0)
    total = take(me).astype(F32)
    for shift in range(1, n):
        arrived = lax.ppermute(take((me + shift) % n), axis, cyclic(axis, shift))
        total = total + arrived.astype(F32)
    return total.astype(BF)


def reduce_gradient(part):
    n, me = lax.axis_size("batch"), lax.axis_index("batch")
    bits = [1 << i for i in range(n.bit_length() - 1)]
    part = halve_columns(part, bits[0])
    half = part.shape[1] // 2
    one, two = part[:, :half], part[:, half:]
    for bit in bits[1:]:
        one = halve_columns(one, bit)
    two = scatter_rows(two, "tm")
    one = scatter_rows(one, "tm")
    for bit in bits[1:]:
        two = halve_columns(two, bit)
    piece = scatter_rows(jnp.concatenate([one, two], axis=1), "space")
    pieces = [piece] + [exchange_bit(piece, "batch", d) for d in range(1, n)]
    placed = [lax.select_n(me ^ b, *pieces) for b in range(n)]
    small = piece.shape[1] // 2

    def ordered(prefix, left):
        if not left:
            return [placed[prefix]]
        return ordered(prefix, left[1:]) + ordered(prefix + left[0], left[1:])

    columns = []
    for first in (0, bits[0]):
        owners = ordered(first, bits[1:])
        columns += [owner[:, :small] for owner in owners] + [owner[:, small:] for owner in owners]
    return jnp.concatenate(columns, axis=1).astype(F32)


def per_device(clip_tokens, frame_order, row_reach, spatial_gain, spatial_heads, spatial_merge,
               temporal_gain, temporal_heads, temporal_merge, cotangent):
    ranks, me = lax.axis_size("tm"), lax.axis_index("tm")
    places, place = lax.axis_size("space"), lax.axis_index("space")
    _, all_frames, rows, part_cols, depth = clip_tokens.shape
    frames, cols = all_frames // ranks, part_cols * ranks
    tokens, span = rows * cols, HALO * cols
    clip = clip_tokens[0]
    pieces = []
    for shift in range(ranks):
        block = lax.dynamic_slice_in_dim(clip, (me + shift) % ranks * frames, frames, 0)
        pieces.append(lax.ppermute(block, "tm", cyclic("tm", shift)) if shift else block)
    here = jnp.stack([lax.select_n((me - j) % ranks, *pieces) if ranks > 2 else
                      jnp.where(me == j, pieces[0], pieces[1]) for j in range(ranks)], axis=2)
    here = here.reshape(frames, rows, cols, depth)
    up = [(i, i + 1) for i in range(places - 1)]
    down = [(i + 1, i) for i in range(places - 1)]
    above = lax.ppermute(here[:, rows - HALO:], "space", up).reshape(frames * span, depth)
    below = lax.ppermute(here[:, :HALO], "space", down).reshape(frames * span, depth)
    flat = here.reshape(frames * tokens, depth)
    projected = jnp.dot(normalize(flat, spatial_gain), spatial_heads, preferred_element_type=F32).astype(BF)
    halo = normalize(jnp.concatenate([above, below]), spatial_gain)
    halo = jnp.dot(halo, spatial_heads[:, depth:], preferred_element_type=F32).astype(BF)
    first_row = (place * rows).astype(jnp.int32).reshape(1)
    context = spatial_attend(projected, halo, row_reach.reshape(-1), first_row, frames, rows, cols, rows * places)
    middle = (flat.astype(F32) + jnp.dot(context, spatial_merge, preferred_element_type=F32)).astype(BF)

    order = frame_order.reshape(-1)
    orders = [lax.dynamic_slice_in_dim(order, (me - shift) % ranks * frames, frames, 0) for shift in range(ranks)]
    arrived = [lax.ppermute(middle, "tm", cyclic("tm", shift)) for shift in range(1, ranks)]
    own = jnp.dot(normalize(middle, temporal_gain), temporal_heads, preferred_element_type=F32).astype(BF)
    others = [jnp.dot(normalize(value, temporal_gain), temporal_heads[:, depth:],
                      preferred_element_type=F32).astype(BF) for value in arrived]
    context = temporal_attend(own, others, orders[0], jnp.concatenate(orders), frames)
    part = lax.dot_general(context, cotangent.reshape(-1, depth), (((0,), (0,)), ((), ())),
                           preferred_element_type=F32).astype(BF)
    weight_grad = reduce_gradient(part)
    output = (middle.astype(F32) + jnp.dot(context, temporal_merge, preferred_element_type=F32)).astype(BF)
    return output.reshape(1, frames, rows, cols, depth), weight_grad


def solution(mesh):
    in_specs = (
        P("batch", None, "space", "tm", None),
        P("batch", None),
        P("batch", "tm"),
        P(),
        P(),
        P(),
        P(),
        P(),
        P(),
        P("batch", "tm", "space", None, None),
    )
    out_specs = (P("batch", "tm", "space", None, None), P(("tm", "space"), None))
    return jax.shard_map(per_device, mesh=mesh, in_specs=in_specs, out_specs=out_specs, check_vma=False)
```

```python
import functools

import jax
import jax.numpy as jnp
from jax import lax
from jax.experimental import pallas as pl
from jax.experimental.pallas import tpu as pltpu
from jax.sharding import PartitionSpec as P

HALO = 4
HEADS = 16
HEAD_DIM = 64
LANES = 128
SCALE = HEAD_DIM ** (-0.5)
FLOOR = 0.5
BF = jnp.bfloat16
F32 = jnp.float32


def normalize(values, gain_vector):
    widened = values.astype(F32)
    scaled = widened * lax.rsqrt(jnp.mean(widened * widened, axis=-1, keepdims=True) + FLOOR)
    return (scaled * gain_vector).astype(BF)


def spatial_kernel(rows, cols, all_rows, reach_ref, first_ref, q_ref, k_ref, v_ref, kt_ref, vt_ref,
                   kb_ref, vb_ref, o_ref, kx, vx, bias):
    frame, block = pl.program_id(0), pl.program_id(1)
    span = HALO * cols
    window = 3 * span
    chunks = rows // HALO

    @pl.when(block == 0)
    def _():
        reach, first = reach_ref[frame], first_ref[0]
        for chunk in range(chunks):
            shape = (span, window)
            q_row = chunk * HALO + lax.broadcasted_iota(jnp.int32, shape, 0) // cols
            k_row = (chunk - 1) * HALO + lax.broadcasted_iota(jnp.int32, shape, 1) // cols
            place = first + k_row
            kept = (jnp.abs(k_row - q_row) <= reach) & (place >= 0) & (place < all_rows)
            bias[chunk] = jnp.where(kept, 0.0, -1e30)

    tokens = rows * cols
    for own, top, low, joined in ((k_ref, kt_ref, kb_ref, kx), (v_ref, vt_ref, vb_ref, vx)):
        joined[:span] = top[...]
        joined[span:span + tokens] = own[...]
        joined[span + tokens:] = low[...]

    lane = lax.broadcasted_iota(jnp.int32, (1, LANES), 1)
    first_head = (lane < HEAD_DIM).astype(F32)
    masks = (first_head.astype(BF), (1.0 - first_head).astype(BF))
    ones = jnp.ones((window, LANES), BF)
    for pair in range(q_ref.shape[1] // LANES):
        at = slice(pair * LANES, (pair + 1) * LANES)
        for chunk in range(chunks):
            here = slice(chunk * span, (chunk + 1) * span)
            near = slice(chunk * span, chunk * span + window)
            q = q_ref[here, at] * BF(SCALE)
            both = jnp.concatenate([q * masks[0], q * masks[1]], axis=0)
            s = lax.dot_general(both, kx[near, at], (((1,), (1,)), ((), ())), preferred_element_type=F32)
            s = s + jnp.concatenate([bias[chunk], bias[chunk]], axis=0)
            p = jnp.exp(s - jnp.max(s, axis=-1, keepdims=True)).astype(BF)
            o = jnp.dot(p, jnp.concatenate([vx[near, at], ones], axis=1), preferred_element_type=F32)
            o = o[:, :LANES] / o[:, LANES:]
            o_ref[here, at] = jnp.where(lane < HEAD_DIM, o[:span], o[span:]).astype(BF)


def spatial_attend(projected, halo, reach, first_row, frames, rows, cols, all_rows):
    depth = projected.shape[1] // 3
    tokens, span = rows * cols, HALO * cols
    width = 2 * LANES
    blocks = depth // width
    here = lambda part: pl.BlockSpec((tokens, width), lambda f, j: (f, part * blocks + j))
    beside = lambda side, part: pl.BlockSpec(
        (span, width), lambda f, j: (side * frames + f, part * blocks + j))
    smem = pl.BlockSpec(memory_space=pltpu.SMEM)
    pairs = frames * HEADS * tokens * 3 * span
    return pl.pallas_call(
        functools.partial(spatial_kernel, rows, cols, all_rows),
        grid=(frames, blocks),
        out_shape=jax.ShapeDtypeStruct((frames * tokens, depth), BF),
        in_specs=[smem, smem, here(0), here(1), here(2), beside(0, 0), beside(0, 1), beside(1, 0), beside(1, 1)],
        out_specs=pl.BlockSpec((tokens, width), lambda f, j: (f, j)),
        scratch_shapes=[
            pltpu.VMEM((tokens + 2 * span, width), BF),
            pltpu.VMEM((tokens + 2 * span, width), BF),
            pltpu.VMEM((rows // HALO, span, 3 * span), F32),
        ],
        cost_estimate=pl.CostEstimate(flops=4 * pairs * LANES, bytes_accessed=frames * tokens * depth * 12,
                                      transcendentals=pairs),
        name="spatial",
    )(reach, first_row, projected, projected, projected, halo, halo, halo, halo)


def temporal_kernel(frames, keys, q_order, k_order, gather_ref, spread_ref, *refs):
    q_refs, k_refs, v_refs, o_ref = refs[:frames], refs[frames:frames + keys], refs[frames + keys:-1], refs[-1]
    for f in range(frames):
        q = q_refs[f][...] * BF(SCALE)
        scores = []
        for g in range(keys):
            s = jnp.dot(q * k_refs[g][...], gather_ref[...], preferred_element_type=F32)
            scores.append(s + jnp.where(k_order[g] <= q_order[f], 0.0, -1e30))
        top_score = functools.reduce(jnp.maximum, scores)
        exps = [jnp.exp(s - top_score) for s in scores]
        scale = 1.0 / functools.reduce(jnp.add, exps)
        total = None
        for g in range(keys):
            w = jnp.dot((exps[g] * scale).astype(BF), spread_ref[...], preferred_element_type=F32)
            term = w * v_refs[g][...].astype(F32)
            total = term if total is None else total + term
        o_ref[f] = total.astype(BF)


def temporal_attend(own, others, q_order, k_order):
    frames, keys = len(own), len(own) + len(others)
    tokens, depth = own[0].shape[0], own[0].shape[1] // 3
    size = min(tokens, 64)
    head = jnp.arange(depth, dtype=jnp.int32) // HEAD_DIM
    gather = (head[:, None] == jnp.arange(LANES, dtype=jnp.int32)[None, :]).astype(BF)
    part = lambda column: pl.BlockSpec((size, depth), lambda i: (i, column))
    smem = pl.BlockSpec(memory_space=pltpu.SMEM)
    whole = lambda shape: pl.BlockSpec(shape, lambda i: (0, 0))
    out = pl.pallas_call(
        functools.partial(temporal_kernel, frames, keys),
        grid=(tokens // size,),
        out_shape=jax.ShapeDtypeStruct((frames, tokens, depth), BF),
        in_specs=[smem, smem, whole((depth, LANES)), whole((LANES, depth))] + [part(0)] * frames
        + [part(1)] * frames + [part(0)] * len(others) + [part(2)] * frames + [part(1)] * len(others),
        out_specs=pl.BlockSpec((frames, size, depth), lambda i: (0, i, 0)),
        cost_estimate=pl.CostEstimate(flops=4 * frames * keys * tokens * depth * LANES,
                                      bytes_accessed=4 * keys * tokens * depth, transcendentals=0),
        name="temporal",
    )(q_order, k_order, gather, gather.T, *own, *own, *others, *own, *others)
    return out.reshape(frames * tokens, depth)


def cyclic(axis, shift):
    n = lax.axis_size(axis)
    return [(i, (i + shift) % n) for i in range(n)]


def exchange_bit(value, axis, bit):
    n = lax.axis_size(axis)
    return lax.ppermute(value, axis, [(i, i ^ bit) for i in range(n)])


def halve_columns(value, bit):
    half = value.shape[1] // 2
    mine = lax.axis_index("batch") // bit % 2
    sent = lax.dynamic_slice_in_dim(value, (1 - mine) * half, half, 1)
    kept = lax.dynamic_slice_in_dim(value, mine * half, half, 1)
    arrived = exchange_bit(sent, "batch", bit)
    return (kept.astype(F32) + arrived.astype(F32)).astype(BF)


def scatter_rows(value, axis):
    n, me = lax.axis_size(axis), lax.axis_index(axis)
    size = value.shape[0] // n
    take = lambda owner: lax.dynamic_slice_in_dim(value, owner * size, size, 0)
    total = take(me).astype(F32)
    for shift in range(1, n):
        arrived = lax.ppermute(take((me + shift) % n), axis, cyclic(axis, shift))
        total = total + arrived.astype(F32)
    return total.astype(BF)


def reduce_gradient(part):
    n, me = lax.axis_size("batch"), lax.axis_index("batch")
    bits = [1 << i for i in range(n.bit_length() - 1)]
    part = halve_columns(part, bits[0])
    half = part.shape[1] // 2
    one, two = part[:, :half], part[:, half:]
    for bit in bits[1:]:
        one = halve_columns(one, bit)
    two = scatter_rows(two, "tm")
    one = scatter_rows(one, "tm")
    for bit in bits[1:]:
        two = halve_columns(two, bit)
    piece = scatter_rows(jnp.concatenate([one, two], axis=1), "space")
    pieces = [piece] + [exchange_bit(piece, "batch", d) for d in range(1, n)]
    placed = [lax.select_n(me ^ b, *pieces) for b in range(n)]
    small = piece.shape[1] // 2

    def ordered(prefix, left):
        if not left:
            return [placed[prefix]]
        return ordered(prefix, left[1:]) + ordered(prefix + left[0], left[1:])

    columns = []
    for first in (0, bits[0]):
        owners = ordered(first, bits[1:])
        columns += [owner[:, :small] for owner in owners] + [owner[:, small:] for owner in owners]
    return jnp.concatenate(columns, axis=1).astype(F32)


def per_device(clip_tokens, frame_order, row_reach, spatial_gain, spatial_heads, spatial_merge,
               temporal_gain, temporal_heads, temporal_merge, cotangent):
    ranks, me = lax.axis_size("tm"), lax.axis_index("tm")
    places, place = lax.axis_size("space"), lax.axis_index("space")
    _, all_frames, rows, part_cols, depth = clip_tokens.shape
    frames, cols = all_frames // ranks, part_cols * ranks
    tokens, span = rows * cols, HALO * cols
    clip = clip_tokens[0]
    up = [(i, i + 1) for i in range(places - 1)]
    down = [(i + 1, i) for i in range(places - 1)]
    first_row = (place * rows).astype(jnp.int32).reshape(1)
    reach = row_reach.reshape(-1)

    def project(values, gain, weights):
        normed = lax.optimization_barrier(normalize(values, gain))
        return jnp.dot(normed, weights, preferred_element_type=F32).astype(BF)

    staged = []
    for f in range(frames):
        pieces = []
        for shift in range(ranks):
            block = lax.dynamic_index_in_dim(clip, (me + shift) % ranks * frames + f, 0, keepdims=False)
            pieces.append(lax.ppermute(block, "tm", cyclic("tm", shift)) if shift else block)
        here = jnp.stack([lax.select_n((me - j) % ranks, *pieces) if ranks > 2 else
                          jnp.where(me == j, pieces[0], pieces[1]) for j in range(ranks)], axis=1)
        here = here.reshape(rows, cols, depth)
        above = lax.ppermute(here[rows - HALO:], "space", up).reshape(span, depth)
        below = lax.ppermute(here[:HALO], "space", down).reshape(span, depth)
        flat = here.reshape(tokens, depth)
        projected = project(flat, spatial_gain, spatial_heads)
        halo = project(jnp.concatenate([above, below]), spatial_gain, spatial_heads[:, depth:])
        staged.append((flat, projected, halo))
    middles = []
    for f, (flat, projected, halo) in enumerate(staged):
        if f:
            middles[-1], projected = lax.optimization_barrier((middles[-1], projected))
        context = spatial_attend(projected, halo, reach[f:f + 1], first_row, 1, rows, cols, rows * places)
        middles.append((flat.astype(F32) + jnp.dot(context, spatial_merge, preferred_element_type=F32)).astype(BF))

    order = frame_order.reshape(-1)
    orders = [lax.dynamic_slice_in_dim(order, (me - shift) % ranks * frames, frames, 0) for shift in range(ranks)]
    arrived = [lax.ppermute(value, "tm", cyclic("tm", shift)) for shift in range(1, ranks) for value in middles]
    own = [project(value, temporal_gain, temporal_heads) for value in middles]
    others = [project(value, temporal_gain, temporal_heads[:, depth:]) for value in arrived]
    context = temporal_attend(own, others, orders[0], jnp.concatenate(orders))
    middle = jnp.concatenate(middles)
    part = lax.dot_general(context, cotangent.reshape(-1, depth), (((0,), (0,)), ((), ())),
                           preferred_element_type=F32).astype(BF)
    weight_grad = reduce_gradient(part)
    output = (middle.astype(F32) + jnp.dot(context, temporal_merge, preferred_element_type=F32)).astype(BF)
    return output.reshape(1, frames, rows, cols, depth), weight_grad


def solution(mesh):
    in_specs = (
        P("batch", None, "space", "tm", None),
        P("batch", None),
        P("batch", "tm"),
        P(),
        P(),
        P(),
        P(),
        P(),
        P(),
        P("batch", "tm", "space", None, None),
    )
    out_specs = (P("batch", "tm", "space", None, None), P(("tm", "space"), None))
    return jax.shard_map(per_device, mesh=mesh, in_specs=in_specs, out_specs=out_specs, check_vma=False)
```

```python
import functools

import jax
import jax.numpy as jnp
from jax import lax
from jax.experimental import pallas as pl
from jax.experimental.pallas import tpu as pltpu
from jax.sharding import PartitionSpec as P

HALO = 4
HEADS = 16
HEAD_DIM = 64
LANES = 128
SCALE = HEAD_DIM ** (-0.5)
FLOOR = 0.5
BF = jnp.bfloat16
F32 = jnp.float32


def normalize(values, gain_vector):
    widened = values.astype(F32)
    scaled = widened * lax.rsqrt(jnp.mean(widened * widened, axis=-1, keepdims=True) + FLOOR)
    return (scaled * gain_vector).astype(BF)


def spatial_kernel(rows, cols, all_rows, reach_ref, first_ref, q_ref, k_ref, v_ref, kt_ref, vt_ref,
                   kb_ref, vb_ref, o_ref, kx, vx, bias):
    frame, block = pl.program_id(0), pl.program_id(1)
    span = HALO * cols
    window = 3 * span
    chunks = rows // HALO

    @pl.when(block == 0)
    def _():
        reach, first = reach_ref[frame], first_ref[0]
        for chunk in range(chunks):
            shape = (span, window)
            q_row = chunk * HALO + lax.broadcasted_iota(jnp.int32, shape, 0) // cols
            k_row = (chunk - 1) * HALO + lax.broadcasted_iota(jnp.int32, shape, 1) // cols
            place = first + k_row
            kept = (jnp.abs(k_row - q_row) <= reach) & (place >= 0) & (place < all_rows)
            bias[chunk] = jnp.where(kept, 0.0, -1e30)

    tokens = rows * cols
    for own, top, low, joined in ((k_ref, kt_ref, kb_ref, kx), (v_ref, vt_ref, vb_ref, vx)):
        joined[:span] = top[...]
        joined[span:span + tokens] = own[...]
        joined[span + tokens:] = low[...]

    lane = lax.broadcasted_iota(jnp.int32, (1, LANES), 1)
    first_head = (lane < HEAD_DIM).astype(F32)
    masks = (first_head.astype(BF), (1.0 - first_head).astype(BF))
    ones = jnp.ones((window, LANES), BF)
    for pair in range(q_ref.shape[1] // LANES):
        at = slice(pair * LANES, (pair + 1) * LANES)
        for chunk in range(chunks):
            here = slice(chunk * span, (chunk + 1) * span)
            near = slice(chunk * span, chunk * span + window)
            q = q_ref[here, at] * BF(SCALE)
            both = jnp.concatenate([q * masks[0], q * masks[1]], axis=0)
            s = lax.dot_general(both, kx[near, at], (((1,), (1,)), ((), ())), preferred_element_type=F32)
            s = s + jnp.concatenate([bias[chunk], bias[chunk]], axis=0)
            p = jnp.exp(s - jnp.max(s, axis=-1, keepdims=True)).astype(BF)
            o = jnp.dot(p, jnp.concatenate([vx[near, at], ones], axis=1), preferred_element_type=F32)
            o = o[:, :LANES] / o[:, LANES:]
            o_ref[here, at] = jnp.where(lane < HEAD_DIM, o[:span], o[span:]).astype(BF)


def spatial_attend(projected, halo, reach, first_row, frame, frames, rows, cols, all_rows):
    depth = projected.shape[1] // 3
    tokens, span = rows * cols, HALO * cols
    width = 2 * LANES
    blocks = depth // width
    here = lambda part: pl.BlockSpec((tokens, width), lambda f, j: (frame + f, part * blocks + j))
    beside = lambda side, part: pl.BlockSpec(
        (span, width), lambda f, j: (side * frames + frame + f, part * blocks + j))
    smem = pl.BlockSpec(memory_space=pltpu.SMEM)
    pairs = HEADS * tokens * 3 * span
    return pl.pallas_call(
        functools.partial(spatial_kernel, rows, cols, all_rows),
        grid=(1, blocks),
        out_shape=jax.ShapeDtypeStruct((tokens, depth), BF),
        in_specs=[smem, smem, here(0), here(1), here(2), beside(0, 0), beside(0, 1), beside(1, 0), beside(1, 1)],
        out_specs=pl.BlockSpec((tokens, width), lambda f, j: (f, j)),
        scratch_shapes=[
            pltpu.VMEM((tokens + 2 * span, width), BF),
            pltpu.VMEM((tokens + 2 * span, width), BF),
            pltpu.VMEM((rows // HALO, span, 3 * span), F32),
        ],
        cost_estimate=pl.CostEstimate(flops=48 * pairs * LANES, bytes_accessed=tokens * depth * 12,
                                      transcendentals=pairs),
        name="spatial",
    )(reach, first_row, projected, projected, projected, halo, halo, halo, halo)


def temporal_kernel(frames, keys, q_order, k_order, gather_ref, spread_ref, *refs):
    q_refs, k_refs, v_refs, o_ref = refs[:frames], refs[frames:frames + keys], refs[frames + keys:-1], refs[-1]
    for f in range(frames):
        q = q_refs[f][...] * BF(SCALE)
        scores = []
        for g in range(keys):
            s = jnp.dot(q * k_refs[g][...], gather_ref[...], preferred_element_type=F32)
            scores.append(s + jnp.where(k_order[g] <= q_order[f], 0.0, -1e30))
        top_score = functools.reduce(jnp.maximum, scores)
        exps = [jnp.exp(s - top_score) for s in scores]
        scale = 1.0 / functools.reduce(jnp.add, exps)
        total = None
        for g in range(keys):
            w = jnp.dot((exps[g] * scale).astype(BF), spread_ref[...], preferred_element_type=F32)
            term = w * v_refs[g][...].astype(F32)
            total = term if total is None else total + term
        o_ref[f] = total.astype(BF)


def temporal_attend(own, others, q_order, k_order):
    frames, keys = len(own), len(own) + len(others)
    tokens, depth = own[0].shape[0], own[0].shape[1] // 3
    size = min(tokens, 64)
    head = jnp.arange(depth, dtype=jnp.int32) // HEAD_DIM
    gather = (head[:, None] == jnp.arange(LANES, dtype=jnp.int32)[None, :]).astype(BF)
    part = lambda column: pl.BlockSpec((size, depth), lambda i: (i, column))
    smem = pl.BlockSpec(memory_space=pltpu.SMEM)
    whole = lambda shape: pl.BlockSpec(shape, lambda i: (0, 0))
    out = pl.pallas_call(
        functools.partial(temporal_kernel, frames, keys),
        grid=(tokens // size,),
        out_shape=jax.ShapeDtypeStruct((frames, tokens, depth), BF),
        in_specs=[smem, smem, whole((depth, LANES)), whole((LANES, depth))] + [part(0)] * frames
        + [part(1)] * frames + [part(0)] * len(others) + [part(2)] * frames + [part(1)] * len(others),
        out_specs=pl.BlockSpec((frames, size, depth), lambda i: (0, i, 0)),
        cost_estimate=pl.CostEstimate(flops=4 * frames * keys * tokens * depth * LANES,
                                      bytes_accessed=4 * keys * tokens * depth, transcendentals=0),
        name="temporal",
    )(q_order, k_order, gather, gather.T, *own, *own, *others, *own, *others)
    return out.reshape(frames * tokens, depth)


def cyclic(axis, shift):
    n = lax.axis_size(axis)
    return [(i, (i + shift) % n) for i in range(n)]


def exchange_bit(value, axis, bit):
    n = lax.axis_size(axis)
    return lax.ppermute(value, axis, [(i, i ^ bit) for i in range(n)])


def halve_columns(value, bit):
    half = value.shape[1] // 2
    mine = lax.axis_index("batch") // bit % 2
    sent = lax.dynamic_slice_in_dim(value, (1 - mine) * half, half, 1)
    kept = lax.dynamic_slice_in_dim(value, mine * half, half, 1)
    arrived = exchange_bit(sent, "batch", bit)
    return (kept.astype(F32) + arrived.astype(F32)).astype(BF)


def scatter_rows(value, axis):
    n, me = lax.axis_size(axis), lax.axis_index(axis)
    size = value.shape[0] // n
    take = lambda owner: lax.dynamic_slice_in_dim(value, owner * size, size, 0)
    total = take(me).astype(F32)
    for shift in range(1, n):
        arrived = lax.ppermute(take((me + shift) % n), axis, cyclic(axis, shift))
        total = total + arrived.astype(F32)
    return total.astype(BF)


def reduce_gradient(part):
    n, me = lax.axis_size("batch"), lax.axis_index("batch")
    bits = [1 << i for i in range(n.bit_length() - 1)]
    part = halve_columns(part, bits[0])
    half = part.shape[1] // 2
    one, two = part[:, :half], part[:, half:]
    for bit in bits[1:]:
        one = halve_columns(one, bit)
    two = scatter_rows(two, "tm")
    one = scatter_rows(one, "tm")
    for bit in bits[1:]:
        two = halve_columns(two, bit)
    piece = scatter_rows(jnp.concatenate([one, two], axis=1), "space")
    pieces = [piece] + [exchange_bit(piece, "batch", d) for d in range(1, n)]
    placed = [lax.select_n(me ^ b, *pieces) for b in range(n)]
    small = piece.shape[1] // 2

    def ordered(prefix, left):
        if not left:
            return [placed[prefix]]
        return ordered(prefix, left[1:]) + ordered(prefix + left[0], left[1:])

    columns = []
    for first in (0, bits[0]):
        owners = ordered(first, bits[1:])
        columns += [owner[:, :small] for owner in owners] + [owner[:, small:] for owner in owners]
    return jnp.concatenate(columns, axis=1).astype(F32)


def per_device(clip_tokens, frame_order, row_reach, spatial_gain, spatial_heads, spatial_merge,
               temporal_gain, temporal_heads, temporal_merge, cotangent):
    ranks, me = lax.axis_size("tm"), lax.axis_index("tm")
    places, place = lax.axis_size("space"), lax.axis_index("space")
    _, all_frames, rows, part_cols, depth = clip_tokens.shape
    frames, cols = all_frames // ranks, part_cols * ranks
    tokens, span = rows * cols, HALO * cols
    clip = clip_tokens[0]
    up = [(i, i + 1) for i in range(places - 1)]
    down = [(i + 1, i) for i in range(places - 1)]
    first_row = (place * rows).astype(jnp.int32).reshape(1)
    reach = row_reach.reshape(-1)

    def project(values, gain, weights):
        return jnp.dot(normalize(values, gain), weights, preferred_element_type=F32).astype(BF)

    pieces = []
    for shift in range(ranks):
        block = lax.dynamic_slice_in_dim(clip, (me + shift) % ranks * frames, frames, 0)
        pieces.append(lax.ppermute(block, "tm", cyclic("tm", shift)) if shift else block)
    here = jnp.stack([lax.select_n((me - j) % ranks, *pieces) if ranks > 2 else
                      jnp.where(me == j, pieces[0], pieces[1]) for j in range(ranks)], axis=2)
    here = here.reshape(frames, rows, cols, depth)
    above = lax.ppermute(here[:, rows - HALO:], "space", up).reshape(frames * span, depth)
    below = lax.ppermute(here[:, :HALO], "space", down).reshape(frames * span, depth)
    flat = here.reshape(frames * tokens, depth)
    projected = project(flat, spatial_gain, spatial_heads)
    halo = project(jnp.concatenate([above, below]), spatial_gain, spatial_heads[:, depth:])
    middles = []
    for f in range(frames):
        reach_now = reach[f:f + 1]
        if f:
            middles[-1], reach_now = lax.optimization_barrier((middles[-1], reach_now))
        context = spatial_attend(projected, halo, reach_now, first_row, f, frames, rows, cols, rows * places)
        middles.append((flat[f * tokens:(f + 1) * tokens].astype(F32)
                        + jnp.dot(context, spatial_merge, preferred_element_type=F32)).astype(BF))

    order = frame_order.reshape(-1)
    orders = [lax.dynamic_slice_in_dim(order, (me - shift) % ranks * frames, frames, 0) for shift in range(ranks)]
    arrived = [lax.ppermute(value, "tm", cyclic("tm", shift)) for shift in range(1, ranks) for value in middles]
    own = [project(value, temporal_gain, temporal_heads) for value in middles]
    others = [project(value, temporal_gain, temporal_heads[:, depth:]) for value in arrived]
    context = temporal_attend(own, others, orders[0], jnp.concatenate(orders))
    middle = jnp.concatenate(middles)
    part = lax.dot_general(context, cotangent.reshape(-1, depth), (((0,), (0,)), ((), ())),
                           preferred_element_type=F32).astype(BF)
    weight_grad = reduce_gradient(part)
    output = (middle.astype(F32) + jnp.dot(context, temporal_merge, preferred_element_type=F32)).astype(BF)
    return output.reshape(1, frames, rows, cols, depth), weight_grad


def solution(mesh):
    in_specs = (
        P("batch", None, "space", "tm", None),
        P("batch", None),
        P("batch", "tm"),
        P(),
        P(),
        P(),
        P(),
        P(),
        P(),
        P("batch", "tm", "space", None, None),
    )
    out_specs = (P("batch", "tm", "space", None, None), P(("tm", "space"), None))
    return jax.shard_map(per_device, mesh=mesh, in_specs=in_specs, out_specs=out_specs, check_vma=False)
```
